32 devices in a mesh: clip: 16 (over z, y, x), mp: 2 (over core).
Axes of the slice: x: 2, y: 2, z: 4, core: 2. Of those that a mesh axis runs over, the one named last changes fastest.
Arguments:
- tokens: bfloat16 [48, 128, 1024], P('clip', None, 'mp'), may hold values from -6 to 6
- bottleneck: bfloat16 [16, 4, 1024], P('clip', None, 'mp'), may hold values from -6 to 6
- clip_lengths: int32 [16], replicated, may hold values from 2 to 4, as said below
- video_blocks: int32 [16], replicated, may hold values from 1 to 3, as said below
- store_map: int32 [16, 3], replicated, may hold values from -1 to 63, as said below
- norm1_gain: float32 [1024], replicated, may hold values from 0.4 to 1.6
- w_qkv: bfloat16 [3, 1024, 1024], P(None, None, 'mp'), may hold values from -0.625 to 0.625
- w_out: bfloat16 [1024, 1024], P('mp'), may hold values from -0.1875 to 0.1875
- norm2_gain: float32 [1024], replicated, may hold values from 0.4 to 1.6
- w_up: bfloat16 [1024, 4096], P(None, 'mp'), may hold values from -0.1875 to 0.1875
- w_down: bfloat16 [4096, 1024], P('mp'), may hold values from -0.09375 to 0.09375
Outputs:
- mixed_tokens: bfloat16 [48, 128, 1024], P('clip', None, 'mp')
- merged_bottleneck: bfloat16 [16, 4, 1024], P('clip', None, 'mp')
The draws below stay inside these ranges and needn't reach their ends.
Inputs may be any that keep to these rules, and one draw needn't show every extreme that they name: clip_lengths[c] counts the blocks of the clip owned by index c of clip. The first video_blocks[c] blocks of clip c are video, the others up to clip_lengths[c] audio; video_blocks[c] <= clip_lengths[c] - 1. store_map[d, s] = c * 4 + b when slot s of device d along clip holds block b of clip c, and -1 when the slot is empty; each block b < clip_lengths[c] of each clip sits in exactly one slot, on a device of the same aligned group of 4 devices along clip as c; no device holds two blocks of one clip.
All inputs are finite; a program needn't handle non-finite values.
Results may differ from the reference program's by a relative error of at most 0.006.
Values may be sent and summed in bfloat16 or wider, within the bound.
A program may use at most 128 MiB of HBM per device.

```python
import jax
import jax.numpy as jnp
from jax import lax

D = 1024
HEADS = 16
FF = 4096
HEAD_DIM = 64
BLK = 128
NB = 4
SLOT_DEV = 4
STORE_DEV = 3
GROUP = 4
CLIPS = 16


def layout(key):
    groups = CLIPS // GROUP
    base = jax.random.fold_in(key, 11)
    keys = [jax.random.fold_in(base, index) for index in range(5)]
    spots = jnp.arange(GROUP, dtype=jnp.int32)
    first = jax.random.randint(keys[0], (groups, GROUP), 0, 1 << 20) * GROUP + spots
    order = jnp.argsort(first, axis=1).astype(jnp.int32)
    ranking = jnp.argsort(order, axis=1).astype(jnp.int32)
    longer = jax.random.randint(keys[1], (groups, GROUP), SLOT_DEV // 2 + 1, SLOT_DEV + 1)
    shorter = jax.random.randint(keys[2], (groups, GROUP), 2, SLOT_DEV // 2 + 1)
    lengths = jnp.where(ranking % 2 == 0, longer, shorter)
    lengths = jnp.where(ranking == 0, SLOT_DEV, lengths).astype(jnp.int32)
    video = (1 + jax.random.randint(keys[3], (groups, GROUP), 0, 1 << 20) % (lengths - 1)).astype(jnp.int32)
    by_rank = jnp.take_along_axis(lengths, order, axis=1)
    ends = jnp.cumsum(by_rank, axis=1).astype(jnp.int32)
    starts = ends - by_rank
    second = jax.random.randint(keys[4], (groups, GROUP), 0, 1 << 20) * GROUP + spots
    residue = jnp.argsort(jnp.argsort(second, axis=1), axis=1).astype(jnp.int32)
    slots = jnp.arange(STORE_DEV, dtype=jnp.int32)
    position = residue[:, :, None] + GROUP * slots[None, None, :]
    owner_rank = jnp.sum((ends[:, None, None, :] <= position[:, :, :, None]).astype(jnp.int32), axis=-1)
    live = owner_rank < GROUP
    safe = jnp.minimum(owner_rank, GROUP - 1).reshape(groups, GROUP * STORE_DEV)
    start_of = jnp.take_along_axis(starts, safe, axis=1).reshape(groups, GROUP, STORE_DEV)
    owner_spot = jnp.take_along_axis(order, safe, axis=1).reshape(groups, GROUP, STORE_DEV)
    owner = owner_spot + GROUP * jnp.arange(groups, dtype=jnp.int32)[:, None, None]
    entry = jnp.where(live, owner * SLOT_DEV + position - start_of, -1).astype(jnp.int32)
    return (lengths.reshape(CLIPS), video.reshape(CLIPS), entry.reshape(CLIPS, STORE_DEV))


def draw_clip_lengths(key, part):
    return layout(key)[0]


def draw_video_blocks(key, part):
    return layout(key)[1]


def draw_store_map(key, part):
    return layout(key)[2]


def draw_w_qkv(key, part):
    raw = jnp.clip(jax.random.normal(jax.random.fold_in(key, 3), (3, D, D), jnp.float32), -4.0, 4.0) * D ** (-0.5)
    return raw.astype(jnp.bfloat16)


def level_of(own_key, extent, cuts, low, high):
    level, own = 1.0, jax.random.fold_in(own_key, 6)
    for dim, shards_of in cuts:
        draws = jnp.exp(jax.random.uniform(jax.random.fold_in(own, dim), (shards_of,), jnp.float32, low / len(cuts), high / len(cuts)))
        level = level * jnp.repeat(draws, extent[dim] // shards_of).reshape([-1 if axis == dim else 1 for axis in range(len(extent))])
    return level


def gaussian(key, shape, deviation, most, shards=(), kind=jnp.bfloat16):
    drawn = deviation * jax.random.normal(key, shape, jnp.float32)
    if shards:
        drawn = drawn * level_of(key, shape, shards, -0.22, 0.18)
    return jnp.clip(drawn, -most, most).astype(kind)


def setup_inputs(seed: int = 0) -> dict:
    seeds = jax.random.split(jax.random.key(seed), 12)
    tokens = gaussian(seeds[0], (CLIPS * STORE_DEV, BLK, D), 1.0, 6.0, ((0, 16), (2, 2)))
    bottleneck = gaussian(seeds[1], (CLIPS, NB, D), 1.0, 6.0, ((0, 16), (2, 2)))
    clip_lengths = draw_clip_lengths(jax.random.fold_in(seeds[11], 71), 0)
    video_blocks = draw_video_blocks(jax.random.fold_in(seeds[11], 71), 0)
    store_map = draw_store_map(jax.random.fold_in(seeds[11], 71), 0)
    norm1_gain = jnp.clip(1.0 + 0.12 * jax.random.normal(seeds[5], (D,), jnp.float32), 0.4, 1.6)
    w_qkv = draw_w_qkv(jax.random.fold_in(seeds[11], 71), 0)
    w_out = gaussian(seeds[7], (D, D), D ** -0.5, 0.1875, ((0, 2),))
    norm2_gain = jnp.clip(1.0 + 0.12 * jax.random.normal(seeds[8], (D,), jnp.float32), 0.4, 1.6)
    w_up = gaussian(seeds[9], (D, FF), D ** -0.5, 0.1875, ((1, 2),))
    w_down = gaussian(seeds[10], (FF, D), FF ** -0.5, 0.09375, ((0, 2),))
    return {"tokens": tokens, "bottleneck": bottleneck, "clip_lengths": clip_lengths, "video_blocks": video_blocks, "store_map": store_map, "norm1_gain": norm1_gain, "w_qkv": w_qkv, "w_out": w_out, "norm2_gain": norm2_gain, "w_up": w_up, "w_down": w_down}


def layer_norm(rows, gain):
    mean = lax.optimization_barrier(jnp.mean(rows, axis=-1, keepdims=True))
    centred = rows - mean
    moment = lax.optimization_barrier(jnp.mean(centred * centred, axis=-1, keepdims=True))
    return centred * lax.rsqrt(moment + 1e-05) * gain.astype(jnp.float32)

def attend(scores, allowed, values):
    masked = jnp.where(allowed, scores, -1e+30)
    top = lax.optimization_barrier(jnp.max(masked, axis=-1, keepdims=True))
    weights = jnp.where(allowed, jnp.exp(masked - top), 0.0)
    weights = (weights / lax.optimization_barrier(jnp.sum(weights, axis=-1, keepdims=True))).astype(jnp.bfloat16)
    return jnp.dot(weights, values, preferred_element_type=jnp.float32)

def reference(tokens, bottleneck, clip_lengths, video_blocks, store_map, norm1_gain, w_qkv, w_out, norm2_gain, w_up, w_down):
    total_rows = SLOT_DEV * BLK
    flat_map = store_map.reshape(-1).astype(jnp.int32)
    target = jnp.where(flat_map >= 0, flat_map, CLIPS * SLOT_DEV).astype(jnp.int32)
    placed = jnp.zeros((CLIPS * SLOT_DEV, BLK, D), tokens.dtype).at[target].set(tokens, mode='drop')
    placed = placed.reshape(CLIPS, total_rows, D)

    def one_clip(items):
        clip_rows, extra, length, video = items
        rows = jnp.concatenate([clip_rows, extra], axis=0)
        normed = layer_norm(rows.astype(jnp.float32), norm1_gain).astype(jnp.bfloat16)
        query = jnp.dot(normed, w_qkv[0], preferred_element_type=jnp.float32).astype(jnp.bfloat16)
        keys = jnp.dot(normed, w_qkv[1], preferred_element_type=jnp.float32).astype(jnp.bfloat16)
        values = jnp.dot(normed, w_qkv[2], preferred_element_type=jnp.float32).astype(jnp.bfloat16)
        block_of = jnp.arange(total_rows, dtype=jnp.int32) // BLK
        token_mode = jnp.where(block_of < video, 0, jnp.where(block_of < length, 1, -1)).astype(jnp.int32)
        key_mode = jnp.concatenate([token_mode, jnp.full((NB,), 2, jnp.int32)])
        token_allow = (key_mode[None, :] == token_mode[:, None]) | (key_mode[None, :] == 2)
        video_allow = jnp.broadcast_to((key_mode == 0) | (key_mode == 2), (NB, total_rows + NB))
        audio_allow = jnp.broadcast_to((key_mode == 1) | (key_mode == 2), (NB, total_rows + NB))
        pieces = []
        for head in range(HEADS):
            cols = slice(head * HEAD_DIM, (head + 1) * HEAD_DIM)
            scores = lax.dot_general(query[:, cols], keys[:, cols], (((1,), (1,)), ((), ())), preferred_element_type=jnp.float32)
            scores = scores * HEAD_DIM ** (-0.5)
            own = attend(scores[:total_rows], token_allow, values[:, cols])
            seen_video = attend(scores[total_rows:], video_allow, values[:, cols])
            seen_audio = attend(scores[total_rows:], audio_allow, values[:, cols])
            pieces.append(jnp.concatenate([own, 0.5 * (seen_video + seen_audio)], axis=0))
        context = jnp.concatenate(pieces, axis=1).astype(jnp.bfloat16)
        after = (rows.astype(jnp.float32) + jnp.dot(context, w_out, preferred_element_type=jnp.float32)).astype(jnp.bfloat16)
        normed2 = layer_norm(after.astype(jnp.float32), norm2_gain).astype(jnp.bfloat16)
        active = jax.nn.gelu(jnp.dot(normed2, w_up, preferred_element_type=jnp.float32), approximate=True).astype(jnp.bfloat16)
        merged = (after.astype(jnp.float32) + jnp.dot(active, w_down, preferred_element_type=jnp.float32)).astype(jnp.bfloat16)
        return (merged[:total_rows], merged[total_rows:])
    merged_rows, merged_extra = lax.map(one_clip, (placed, bottleneck, clip_lengths, video_blocks))
    merged_rows = merged_rows.reshape(CLIPS * SLOT_DEV, BLK, D)
    picked = merged_rows[jnp.maximum(flat_map, 0)]
    mixed_tokens = jnp.where(flat_map[:, None, None] >= 0, picked, jnp.zeros_like(picked))
    return (mixed_tokens, merged_extra)
```

```python
import functools

import jax
import jax.numpy as jnp
from jax import lax
from jax.experimental import pallas as pl
from jax.experimental.pallas import tpu as pltpu
from jax.sharding import PartitionSpec as P

HEAD_DIM = 64
GROUP = 4
EPS = 1e-05
NEG = -1e30
EXTRA = 16
BF16 = jnp.bfloat16
F32 = jnp.float32


def layer_norm(halves, gain):
    x = jnp.concatenate([h.astype(F32) for h in halves], axis=1)
    mean = jnp.mean(x, axis=-1, keepdims=True)
    centred = x - mean
    moment = jnp.mean(centred * centred, axis=-1, keepdims=True)
    return (centred * lax.rsqrt(moment + EPS) * gain).astype(BF16)


def dot(a, b):
    return jnp.dot(a, b, preferred_element_type=F32)


def kernel(
    blk,
    nb,
    video_ref,
    map_ref,
    tok_hbm,
    bot_ref,
    g1_ref,
    g2_ref,
    wqkv_hbm,
    wout_hbm,
    wup_hbm,
    wdown_hbm,
    out_ref,
    outb_ref,
    tok,
    wqkv,
    wout,
    wup,
    wdown,
    snd,
    x,
    ext,
    q,
    k,
    v,
    ctx,
    bias,
    ps1,
    pr1,
    own1,
    aft,
    act,
    ps2,
    pr2,
    own2,
    fin,
    ret,
    ld_sem,
    send_sem,
    recv_sem,
):
    slots = tok.shape[0]
    width = tok.shape[2]
    pairs = q.shape[0]
    keys = k.shape[1]
    rows = x.shape[1]
    ff = wup.shape[1]
    total = GROUP * blk

    me = lax.axis_index("clip")
    core = lax.axis_index("mp")
    peer = 1 - core
    bit0 = lax.rem(me, 2)
    bit1 = lax.rem(lax.div(me, 2), 2)
    flip0 = 1 - 2 * bit0
    flip1 = 2 - 4 * bit1
    partner = [me, me + flip0, me + flip1, me + flip0 + flip1]

    loads = [pltpu.make_async_copy(tok_hbm, tok, ld_sem.at[0])]
    loads.append(pltpu.make_async_copy(wqkv_hbm, wqkv, ld_sem.at[1]))
    for h in range(2):
        cols = pl.ds(h * width, width)
        loads.append(pltpu.make_async_copy(wout_hbm.at[:, cols], wout.at[h], ld_sem.at[2 + h]))
    loads.append(pltpu.make_async_copy(wup_hbm, wup, ld_sem.at[4]))
    for h in range(2):
        cols = pl.ds(h * width, width)
        loads.append(pltpu.make_async_copy(wdown_hbm.at[:, cols], wdown.at[h], ld_sem.at[5 + h]))
    for load in loads:
        load.start()

    barrier = pltpu.get_barrier_semaphore()
    for r in range(1, GROUP):
        pl.semaphore_signal(barrier, inc=1, device_id={"clip": partner[r]})
    pl.semaphore_signal(barrier, inc=1, device_id={"mp": peer})

    entry = [map_ref[me, s] for s in range(slots)]
    own = [jnp.where(e >= 0, lax.div(e, GROUP), -1) for e in entry]
    pick = []
    for r in range(GROUP):
        chosen = jnp.int32(0)
        for s in range(slots):
            chosen = jnp.where(own[s] == partner[r], s, chosen)
        pick.append(chosen)
    video = video_ref[me]
    mode = []
    for r in range(GROUP):
        m = jnp.int32(-1)
        for s in range(slots):
            e = map_ref[partner[r], s]
            mine = (e >= 0) & (lax.div(e, GROUP) == me)
            m = jnp.where(mine, jnp.where(lax.rem(e, GROUP) < video, 0, 1), m)
        mode.append(m)

    place = [(GROUP - 1) * blk] + [(r - 1) * blk for r in range(1, GROUP)]
    span = [pl.ds(place[0], blk + EXTRA)] + [pl.ds(place[r], blk) for r in range(1, GROUP)]
    size = [blk + EXTRA] + [blk] * (GROUP - 1)

    def ici(r, src, dst, base):
        return pltpu.make_async_remote_copy(
            src_ref=src,
            dst_ref=dst,
            send_sem=send_sem.at[base + r],
            recv_sem=recv_sem.at[base + r],
            device_id={"clip": partner[r]},
        )

    def d2d(r, src, dst, base):
        return pltpu.make_async_remote_copy(
            src_ref=src,
            dst_ref=dst,
            send_sem=send_sem.at[base + r],
            recv_sem=recv_sem.at[base + r],
            device_id={"mp": peer},
        )

    half = x.at[core]
    arrive = [ici(r, snd.at[r - 1], half.at[span[r]], 0) if r else None for r in range(GROUP)]
    share = [d2d(r, half.at[span[r]], half.at[span[r]], 4) for r in range(GROUP)]
    proj = [d2d(r, ps1.at[span[r]], pr1.at[span[r]], 8) for r in range(GROUP)]
    joined = [d2d(r, aft.at[core].at[span[r]], aft.at[core].at[span[r]], 12) for r in range(GROUP)]
    down = [d2d(r, ps2.at[span[r]], pr2.at[span[r]], 16) for r in range(GROUP)]
    back = [ici(r, fin.at[r - 1], ret.at[r], 20) if r else None for r in range(GROUP)]

    loads[0].wait()
    for r in range(1, GROUP):
        snd[r - 1] = tok[pick[r]]
    x[core, pl.ds(place[0], blk)] = tok[pick[0]]
    small = bot_ref[0].astype(F32)
    for i in range(EXTRA // nb):
        ext[pl.ds(i * nb, nb)] = small
    x[core, pl.ds(total, EXTRA)] = ext[...].astype(BF16)

    pl.semaphore_wait(barrier, GROUP)
    for r in (1, 2, 3):
        arrive[r].start()
    share[0].start()

    column = lax.broadcasted_iota(jnp.int32, (1, keys), 1)
    extra_key = (column >= total) & (column < total + nb)
    key_mode = jnp.full((1, keys), -1, jnp.int32)
    for r in range(GROUP):
        inside = (column >= place[r]) & (column < place[r] + blk)
        key_mode = jnp.where(inside, mode[r], key_mode)

    def bias_of(m):
        return jnp.where(extra_key | ((key_mode == m) & (key_mode >= 0)), 0.0, NEG).astype(F32)

    row_bias = [bias_of(mode[r]) for r in range(GROUP)]
    bias[pl.ds(0, blk)] = jnp.broadcast_to(row_bias[0], (blk, keys))
    line = lax.broadcasted_iota(jnp.int32, (EXTRA, keys), 0)
    bias[pl.ds(blk, EXTRA)] = jnp.where(
        (line >= nb) & (line < 2 * nb),
        jnp.broadcast_to(bias_of(1), (EXTRA, keys)),
        jnp.broadcast_to(bias_of(0), (EXTRA, keys)),
    )
    for j in range(pairs):
        k[j, pl.ds(rows, keys - rows)] = jnp.zeros((keys - rows, 128), BF16)
        v[j, pl.ds(rows, keys - rows)] = jnp.zeros((keys - rows, 128), BF16)

    def project(r):
        n = layer_norm([x[0, span[r]], x[1, span[r]]], g1_ref[...])
        for i, target in enumerate((q, k, v)):
            y = dot(n, wqkv[i])
            if i == 0:
                y = y.astype(BF16).astype(F32) * HEAD_DIM ** (-0.5)
            y = y.astype(BF16)
            for j in range(pairs):
                target[j, span[r]] = y[:, j * 128 : (j + 1) * 128]

    loads[1].wait()
    share[0].wait_recv()
    project(0)
    for r in (1, 2):
        arrive[r].wait_recv()
        share[r].start()
    for r in (1, 2):
        share[r].wait_recv()
        project(r)
    arrive[3].wait_recv()
    share[3].start()
    share[3].wait_recv()
    project(3)

    def attend(r):
        lane = lax.broadcasted_iota(jnp.int32, (1, 128), 1)

        def step(j, _):
            qs = q[j, span[r]]
            ks = k[j]
            vs = v[j]
            outs = []
            for h in range(2):
                sel = (lane < HEAD_DIM) if h == 0 else (lane >= HEAD_DIM)
                qh = jnp.where(sel, qs, jnp.zeros_like(qs))
                s = lax.dot_general(qh, ks, (((1,), (1,)), ((), ())), preferred_element_type=F32)
                s = s + (bias[...] if r == 0 else row_bias[r])
                top = jnp.max(s, axis=-1, keepdims=True)
                p = jnp.exp(s - top)
                norm = jnp.sum(p, axis=-1, keepdims=True)
                outs.append(dot(p.astype(BF16), vs) / norm)
            o = jnp.where(lane < HEAD_DIM, outs[0], outs[1])
            if r == 0:
                ctx[j, pl.ds(place[0], blk)] = o[:blk].astype(BF16)
                e = o[blk:]
                e = 0.5 * (e + pltpu.roll(e, EXTRA - nb, 0))
                ctx[j, pl.ds(total, EXTRA)] = e.astype(BF16)
            else:
                ctx[j, span[r]] = o.astype(BF16)
            return 0

        lax.fori_loop(0, pairs, step, 0)

    def stage_a(r):
        attend(r)
        c = jnp.concatenate([ctx[j, span[r]] for j in range(pairs)], axis=1)
        ps1[span[r]] = dot(c, wout[peer]).astype(BF16)
        proj[r].start()
        own1[span[r]] = dot(c, wout[core])

    def stage_b(r):
        proj[r].wait_recv()
        total_sum = x[core, span[r]].astype(F32) + (own1[span[r]] + pr1[span[r]].astype(F32))
        aft[core, span[r]] = total_sum.astype(BF16)
        joined[r].start()

    def stage_c(r):
        joined[r].wait_recv()
        n = layer_norm([aft[0, span[r]], aft[1, span[r]]], g2_ref[...])
        tile = width
        for t in range(ff // tile):
            up = dot(n, wup[:, t * tile : (t + 1) * tile])
            act[pl.ds(0, size[r]), t * tile : (t + 1) * tile] = jax.nn.gelu(up, approximate=True).astype(BF16)
        a = act[pl.ds(0, size[r])]
        ps2[span[r]] = dot(a, wdown[peer]).astype(BF16)
        down[r].start()
        own2[span[r]] = dot(a, wdown[core])

    def stage_d(r):
        down[r].wait_recv()
        merged = aft[core, span[r]].astype(F32) + (own2[span[r]] + pr2[span[r]].astype(F32))
        if r == 0:
            ret[0] = merged[:blk].astype(BF16)
            outb_ref[0] = merged[blk : blk + nb].astype(BF16)
        else:
            fin[r - 1] = merged.astype(BF16)
            back[r].start()

    loads[2].wait()
    loads[3].wait()
    stage_a(3)
    stage_a(1)
    stage_b(3)
    stage_a(2)
    stage_b(1)
    for load in loads[4:]:
        load.wait()
    stage_c(3)
    stage_a(0)
    stage_b(2)
    stage_d(3)
    stage_c(1)
    stage_b(0)
    stage_d(1)
    stage_c(2)
    stage_d(2)
    stage_c(0)
    stage_d(0)
    for r in (3, 1, 2):
        back[r].wait_recv()
    for s in range(slots):
        where = jnp.int32(0)
        for r in range(GROUP):
            where = jnp.where(own[s] == partner[r], r, where)
        live = jnp.where(entry[s] >= 0, 1.0, 0.0).astype(F32)
        block = ret[where].astype(F32)
        out_ref[s] = (block * live).astype(BF16)
    for r in range(1, GROUP):
        arrive[r].wait_send()
        back[r].wait_send()
    for r in range(GROUP):
        for c in (share, proj, joined, down):
            c[r].wait_send()


def body(
    tokens,
    bottleneck,
    clip_lengths,
    video_blocks,
    store_map,
    norm1_gain,
    w_qkv,
    w_out,
    norm2_gain,
    w_up,
    w_down,
):
    slots, blk, width = tokens.shape
    nb = bottleneck.shape[1]
    dim = w_qkv.shape[1]
    inner = w_qkv.shape[2]
    ff = w_up.shape[1]
    pairs = inner // 128
    rows = GROUP * blk + EXTRA
    keys = (rows + 127) // 128 * 128
    smem = pl.BlockSpec(memory_space=pltpu.SMEM)
    vmem = pl.BlockSpec(memory_space=pltpu.VMEM)
    hbm = pl.BlockSpec(memory_space=pl.ANY)
    V = pltpu.VMEM
    return pl.pallas_call(
        functools.partial(kernel, blk, nb),
        out_shape=(
            jax.ShapeDtypeStruct(tokens.shape, BF16),
            jax.ShapeDtypeStruct(bottleneck.shape, BF16),
        ),
        in_specs=[smem, smem, hbm, vmem, vmem, vmem, hbm, hbm, hbm, hbm],
        out_specs=(vmem, vmem),
        scratch_shapes=[
            V((slots, blk, width), BF16),
            V(w_qkv.shape, BF16),
            V((2, inner, width), BF16),
            V(w_up.shape, BF16),
            V((2, ff, width), BF16),
            V((GROUP - 1, blk, width), BF16),
            V((2, rows, width), BF16),
            V((EXTRA, width), F32),
            V((pairs, rows, 128), BF16),
            V((pairs, keys, 128), BF16),
            V((pairs, keys, 128), BF16),
            V((pairs, rows, 128), BF16),
            V((blk + EXTRA, keys), F32),
            V((rows, width), BF16),
            V((rows, width), BF16),
            V((rows, width), F32),
            V((2, rows, width), BF16),
            V((blk + EXTRA, ff), BF16),
            V((rows, width), BF16),
            V((rows, width), BF16),
            V((rows, width), F32),
            V((GROUP - 1, blk, width), BF16),
            V((GROUP, blk, width), BF16),
            pltpu.SemaphoreType.DMA((7,)),
            pltpu.SemaphoreType.DMA((24,)),
            pltpu.SemaphoreType.DMA((24,)),
        ],
        compiler_params=pltpu.CompilerParams(collective_id=0, has_side_effects=True),
        name="merge_layer",
    )(
        video_blocks,
        store_map,
        tokens,
        bottleneck,
        norm1_gain.reshape(1, dim),
        norm2_gain.reshape(1, dim),
        w_qkv,
        w_out,
        w_up,
        w_down,
    )


def solution(mesh):
    placed = (
        P("clip", None, "mp"),
        P("clip", None, "mp"),
        P(),
        P(),
        P(),
        P(),
        P(None, None, "mp"),
        P("mp", None),
        P(),
        P(None, "mp"),
        P("mp", None),
    )
    return jax.shard_map(
        body,
        mesh=mesh,
        in_specs=placed,
        out_specs=(P("clip", None, "mp"), P("clip", None, "mp")),
        check_vma=False,
    )
```

```python
import functools

import jax
import jax.numpy as jnp
from jax import lax
from jax.experimental import pallas as pl
from jax.experimental.pallas import tpu as pltpu
from jax.sharding import PartitionSpec as P

HEAD_DIM = 64
GROUP = 4
EPS = 1e-05
NEG = -1e30
EXTRA = 16
UNROLL = True
BF16 = jnp.bfloat16
F32 = jnp.float32


def layer_norm(halves, gain):
    x = jnp.concatenate([h.astype(F32) for h in halves], axis=1)
    mean = jnp.mean(x, axis=-1, keepdims=True)
    centred = x - mean
    moment = jnp.mean(centred * centred, axis=-1, keepdims=True)
    return (centred * lax.rsqrt(moment + EPS) * gain).astype(BF16)


def dot(a, b):
    return jnp.dot(a, b, preferred_element_type=F32)


def kernel(
    blk,
    nb,
    video_ref,
    map_ref,
    tok_hbm,
    bot_ref,
    g1_ref,
    g2_ref,
    wqkv_hbm,
    wout_hbm,
    wup_hbm,
    wdown_hbm,
    out_ref,
    outb_ref,
    tok,
    wqkv,
    wout,
    wup,
    wdown,
    snd,
    x,
    ext,
    q,
    k,
    v,
    ctx,
    bias,
    ps1,
    pr1,
    own1,
    aft,
    act,
    ps2,
    pr2,
    own2,
    fin,
    ret,
    ld_sem,
    send_sem,
    recv_sem,
):
    slots = tok.shape[0]
    width = tok.shape[2]
    pairs = q.shape[0]
    keys = k.shape[1]
    rows = x.shape[1]
    ff = wup.shape[1]
    total = GROUP * blk

    me = lax.axis_index("clip")
    core = lax.axis_index("mp")
    peer = 1 - core
    bit0 = lax.rem(me, 2)
    bit1 = lax.rem(lax.div(me, 2), 2)
    flip0 = 1 - 2 * bit0
    flip1 = 2 - 4 * bit1
    partner = [me, me + flip0, me + flip1, me + flip0 + flip1]

    loads = [pltpu.make_async_copy(tok_hbm, tok, ld_sem.at[0])]
    loads.append(pltpu.make_async_copy(wqkv_hbm, wqkv, ld_sem.at[1]))
    for h in range(2):
        cols = pl.ds(h * width, width)
        loads.append(pltpu.make_async_copy(wout_hbm.at[:, cols], wout.at[h], ld_sem.at[2 + h]))
    loads.append(pltpu.make_async_copy(wup_hbm, wup, ld_sem.at[4]))
    for h in range(2):
        cols = pl.ds(h * width, width)
        loads.append(pltpu.make_async_copy(wdown_hbm.at[:, cols], wdown.at[h], ld_sem.at[5 + h]))
    for load in loads:
        load.start()

    barrier = pltpu.get_barrier_semaphore()
    for r in range(1, GROUP):
        pl.semaphore_signal(barrier, inc=1, device_id={"clip": partner[r]})
    pl.semaphore_signal(barrier, inc=1, device_id={"mp": peer})

    entry = [map_ref[s, me] for s in range(slots)]
    own = [jnp.where(e >= 0, lax.div(e, GROUP), -1) for e in entry]
    pick = []
    for r in range(GROUP):
        chosen = jnp.int32(0)
        for s in range(slots):
            chosen = jnp.where(own[s] == partner[r], s, chosen)
        pick.append(chosen)
    video = video_ref[me]
    mode = []
    for r in range(GROUP):
        m = jnp.int32(-1)
        for s in range(slots):
            e = map_ref[s, partner[r]]
            mine = (e >= 0) & (lax.div(e, GROUP) == me)
            m = jnp.where(mine, jnp.where(lax.rem(e, GROUP) < video, 0, 1), m)
        mode.append(m)

    place = [(GROUP - 1) * blk] + [(r - 1) * blk for r in range(1, GROUP)]
    span = [pl.ds(place[0], blk + EXTRA)] + [pl.ds(place[r], blk) for r in range(1, GROUP)]
    size = [blk + EXTRA] + [blk] * (GROUP - 1)

    def ici(r, src, dst, base):
        return pltpu.make_async_remote_copy(
            src_ref=src,
            dst_ref=dst,
            send_sem=send_sem.at[base + r],
            recv_sem=recv_sem.at[base + r],
            device_id={"clip": partner[r]},
        )

    def d2d(r, src, dst, base):
        return pltpu.make_async_remote_copy(
            src_ref=src,
            dst_ref=dst,
            send_sem=send_sem.at[base + r],
            recv_sem=recv_sem.at[base + r],
            device_id={"mp": peer},
        )

    half = x.at[core]
    arrive = [ici(r, snd.at[r - 1], half.at[span[r]], 0) if r else None for r in range(GROUP)]
    share = [d2d(r, half.at[span[r]], half.at[span[r]], 4) for r in range(GROUP)]
    proj = [d2d(r, ps1.at[span[r]], pr1.at[span[r]], 8) for r in range(GROUP)]
    joined = [d2d(r, aft.at[core].at[span[r]], aft.at[core].at[span[r]], 12) for r in range(GROUP)]
    down = [d2d(r, ps2.at[span[r]], pr2.at[span[r]], 16) for r in range(GROUP)]
    back = [ici(r, fin.at[r - 1], ret.at[r], 20) if r else None for r in range(GROUP)]

    loads[0].wait()
    for r in range(1, GROUP):
        snd[r - 1] = tok[pick[r]]
    x[core, pl.ds(place[0], blk)] = tok[pick[0]]
    small = bot_ref[0].astype(F32)
    for i in range(EXTRA // nb):
        ext[pl.ds(i * nb, nb)] = small
    x[core, pl.ds(total, EXTRA)] = ext[...].astype(BF16)

    pl.semaphore_wait(barrier, GROUP)
    for r in (1, 2, 3):
        arrive[r].start()
    share[0].start()

    column = lax.broadcasted_iota(jnp.int32, (1, keys), 1)
    extra_key = (column >= total) & (column < total + nb)
    key_mode = jnp.full((1, keys), -1, jnp.int32)
    for r in range(GROUP):
        inside = (column >= place[r]) & (column < place[r] + blk)
        key_mode = jnp.where(inside, mode[r], key_mode)

    def bias_of(m):
        return jnp.where(extra_key | ((key_mode == m) & (key_mode >= 0)), 0.0, NEG).astype(F32)

    row_bias = [bias_of(mode[r]) for r in range(GROUP)]
    bias[pl.ds(0, blk)] = jnp.broadcast_to(row_bias[0], (blk, keys))
    line = lax.broadcasted_iota(jnp.int32, (EXTRA, keys), 0)
    bias[pl.ds(blk, EXTRA)] = jnp.where(
        (line >= nb) & (line < 2 * nb),
        jnp.broadcast_to(bias_of(1), (EXTRA, keys)),
        jnp.broadcast_to(bias_of(0), (EXTRA, keys)),
    )
    for j in range(pairs):
        k[j, pl.ds(rows, keys - rows)] = jnp.zeros((keys - rows, 128), BF16)
        v[j, pl.ds(rows, keys - rows), :128] = jnp.zeros((keys - rows, 128), BF16)
        v[j, :, 128:] = jnp.ones((keys, 128), BF16)

    def project(r):
        n = layer_norm([x[0, span[r]], x[1, span[r]]], g1_ref[...])
        for i, target in enumerate((q, k, v)):
            y = dot(n, wqkv[i])
            if i == 0:
                y = y.astype(BF16).astype(F32) * HEAD_DIM ** (-0.5)
            y = y.astype(BF16)
            for j in range(pairs):
                target[j, span[r], :128] = y[:, j * 128 : (j + 1) * 128]

    loads[1].wait()
    share[0].wait_recv()
    project(0)
    for r in (1, 2):
        arrive[r].wait_recv()
        share[r].start()
    for r in (1, 2):
        share[r].wait_recv()
        project(r)
    arrive[3].wait_recv()
    share[3].start()
    share[3].wait_recv()
    project(3)

    def attend(r):
        lane = lax.broadcasted_iota(jnp.int32, (1, 128), 1)
        low = lane < HEAD_DIM

        def step(j, _):
            qs = q[j, span[r]]
            zero = jnp.zeros_like(qs)
            both = jnp.concatenate([jnp.where(low, qs, zero), jnp.where(low, zero, qs)], axis=0)
            s = lax.dot_general(both, k[j], (((1,), (1,)), ((), ())), preferred_element_type=F32)
            if r == 0:
                b = bias[...]
                s = s + jnp.concatenate([b, b], axis=0)
            else:
                s = s + row_bias[r]
            top = jnp.max(s, axis=-1, keepdims=True)
            p = jnp.exp(s - top).astype(BF16)
            o = dot(p, v[j])
            m = size[r]
            over = jnp.where(low, o[:m, :128], o[m:, :128])
            under = jnp.where(low, o[:m, 128:], o[m:, 128:])
            o = over / under
            if r == 0:
                ctx[j, pl.ds(place[0], blk)] = o[:blk].astype(BF16)
                e = o[blk:]
                e = 0.5 * (e + pltpu.roll(e, EXTRA - nb, 0))
                ctx[j, pl.ds(total, EXTRA)] = e.astype(BF16)
            else:
                ctx[j, span[r]] = o.astype(BF16)
            return 0

        lax.fori_loop(0, pairs, step, 0, unroll=UNROLL)

    def stage_a(r):
        attend(r)
        c = jnp.concatenate([ctx[j, span[r]] for j in range(pairs)], axis=1)
        ps1[span[r]] = dot(c, wout[peer]).astype(BF16)
        proj[r].start()
        own1[span[r]] = dot(c, wout[core])

    def stage_b(r):
        proj[r].wait_recv()
        total_sum = x[core, span[r]].astype(F32) + (own1[span[r]] + pr1[span[r]].astype(F32))
        aft[core, span[r]] = total_sum.astype(BF16)
        joined[r].start()

    def stage_c(r):
        joined[r].wait_recv()
        n = layer_norm([aft[0, span[r]], aft[1, span[r]]], g2_ref[...])
        tile = width
        for t in range(ff // tile):
            up = dot(n, wup[:, t * tile : (t + 1) * tile])
            act[pl.ds(0, size[r]), t * tile : (t + 1) * tile] = jax.nn.gelu(up, approximate=True).astype(BF16)
        a = act[pl.ds(0, size[r])]
        ps2[span[r]] = dot(a, wdown[peer]).astype(BF16)
        down[r].start()
        own2[span[r]] = dot(a, wdown[core])

    def stage_d(r):
        down[r].wait_recv()
        merged = aft[core, span[r]].astype(F32) + (own2[span[r]] + pr2[span[r]].astype(F32))
        if r == 0:
            ret[0] = merged[:blk].astype(BF16)
            outb_ref[0] = merged[blk : blk + nb].astype(BF16)
        else:
            fin[r - 1] = merged.astype(BF16)
            back[r].start()

    loads[2].wait()
    loads[3].wait()
    stage_a(3)
    stage_a(1)
    stage_b(3)
    stage_a(2)
    stage_b(1)
    for load in loads[4:]:
        load.wait()
    stage_c(3)
    stage_a(0)
    stage_b(2)
    stage_d(3)
    stage_c(1)
    stage_b(0)
    stage_d(1)
    stage_c(2)
    stage_d(2)
    stage_c(0)
    stage_d(0)
    for r in (3, 1, 2):
        back[r].wait_recv()
    for s in range(slots):
        where = jnp.int32(0)
        for r in range(GROUP):
            where = jnp.where(own[s] == partner[r], r, where)
        live = jnp.where(entry[s] >= 0, 1.0, 0.0).astype(F32)
        block = ret[where].astype(F32)
        out_ref[s] = (block * live).astype(BF16)
    for r in range(1, GROUP):
        arrive[r].wait_send()
        back[r].wait_send()
    for r in range(GROUP):
        for c in (share, proj, joined, down):
            c[r].wait_send()


def body(
    tokens,
    bottleneck,
    clip_lengths,
    video_blocks,
    store_map,
    norm1_gain,
    w_qkv,
    w_out,
    norm2_gain,
    w_up,
    w_down,
):
    slots, blk, width = tokens.shape
    nb = bottleneck.shape[1]
    dim = w_qkv.shape[1]
    inner = w_qkv.shape[2]
    ff = w_up.shape[1]
    pairs = inner // 128
    rows = GROUP * blk + EXTRA
    keys = (rows + 127) // 128 * 128
    smem = pl.BlockSpec(memory_space=pltpu.SMEM)
    vmem = pl.BlockSpec(memory_space=pltpu.VMEM)
    hbm = pl.BlockSpec(memory_space=pl.ANY)
    V = pltpu.VMEM
    return pl.pallas_call(
        functools.partial(kernel, blk, nb),
        out_shape=(
            jax.ShapeDtypeStruct(tokens.shape, BF16),
            jax.ShapeDtypeStruct(bottleneck.shape, BF16),
        ),
        in_specs=[smem, smem, hbm, vmem, vmem, vmem, hbm, hbm, hbm, hbm],
        out_specs=(vmem, vmem),
        scratch_shapes=[
            V((slots, blk, width), BF16),
            V(w_qkv.shape, BF16),
            V((2, inner, width), BF16),
            V(w_up.shape, BF16),
            V((2, ff, width), BF16),
            V((GROUP - 1, blk, width), BF16),
            V((2, rows, width), BF16),
            V((EXTRA, width), F32),
            V((pairs, rows, 128), BF16),
            V((pairs, keys, 128), BF16),
            V((pairs, keys, 256), BF16),
            V((pairs, rows, 128), BF16),
            V((blk + EXTRA, keys), F32),
            V((rows, width), BF16),
            V((rows, width), BF16),
            V((rows, width), F32),
            V((2, rows, width), BF16),
            V((blk + EXTRA, ff), BF16),
            V((rows, width), BF16),
            V((rows, width), BF16),
            V((rows, width), F32),
            V((GROUP - 1, blk, width), BF16),
            V((GROUP, blk, width), BF16),
            pltpu.SemaphoreType.DMA((7,)),
            pltpu.SemaphoreType.DMA((24,)),
            pltpu.SemaphoreType.DMA((24,)),
        ],
        compiler_params=pltpu.CompilerParams(collective_id=0, has_side_effects=True),
        name="merge_layer",
    )(
        video_blocks,
        store_map.T,
        tokens,
        bottleneck,
        norm1_gain.reshape(1, dim),
        norm2_gain.reshape(1, dim),
        w_qkv,
        w_out,
        w_up,
        w_down,
    )


def solution(mesh):
    placed = (
        P("clip", None, "mp"),
        P("clip", None, "mp"),
        P(),
        P(),
        P(),
        P(),
        P(None, None, "mp"),
        P("mp", None),
        P(),
        P(None, "mp"),
        P("mp", None),
    )
    return jax.shard_map(
        body,
        mesh=mesh,
        in_specs=placed,
        out_specs=(P("clip", None, "mp"), P("clip", None, "mp")),
        check_vma=False,
    )
```

```python
import functools

import jax
import jax.numpy as jnp
from jax import lax
from jax.experimental import pallas as pl
from jax.experimental.pallas import tpu as pltpu
from jax.sharding import PartitionSpec as P

HEAD_DIM = 64
GROUP = 4
EPS = 1e-05
NEG = -1e30
EXTRA = 16
UNROLL = True
BF16 = jnp.bfloat16
F32 = jnp.float32


def layer_norm(halves, gain):
    x = jnp.concatenate([h.astype(F32) for h in halves], axis=1)
    mean = jnp.mean(x, axis=-1, keepdims=True)
    centred = x - mean
    moment = jnp.mean(centred * centred, axis=-1, keepdims=True)
    return (centred * lax.rsqrt(moment + EPS) * gain).astype(BF16)


def dot(a, b):
    return jnp.dot(a, b, preferred_element_type=F32)


def kernel(
    blk,
    nb,
    video_ref,
    map_ref,
    tok_hbm,
    bot_ref,
    g1_ref,
    g2_ref,
    wqkv_hbm,
    wout_hbm,
    wup_hbm,
    wdown_hbm,
    out_ref,
    outb_ref,
    tok,
    wqkv,
    wout,
    wup,
    wdown,
    snd,
    x,
    ext,
    q,
    k,
    v,
    ctx,
    bias,
    ps1,
    pr1,
    own1,
    aft,
    act,
    ps2,
    pr2,
    own2,
    fin,
    ret,
    ld_sem,
    send_sem,
    recv_sem,
):
    slots = tok.shape[0]
    width = tok.shape[2]
    pairs = q.shape[0]
    keys = k.shape[1]
    rows = x.shape[1]
    ff = wup.shape[1]
    total = GROUP * blk

    me = lax.axis_index("clip")
    core = lax.axis_index("mp")
    peer = 1 - core
    bit0 = lax.rem(me, 2)
    bit1 = lax.rem(lax.div(me, 2), 2)
    flip0 = 1 - 2 * bit0
    flip1 = 2 - 4 * bit1
    partner = [me, me + flip0, me + flip1, me + flip0 + flip1]

    loads = [pltpu.make_async_copy(tok_hbm, tok, ld_sem.at[0])]
    loads.append(pltpu.make_async_copy(wqkv_hbm, wqkv, ld_sem.at[1]))
    for h in range(2):
        cols = pl.ds(h * width, width)
        loads.append(pltpu.make_async_copy(wout_hbm.at[:, cols], wout.at[h], ld_sem.at[2 + h]))
    loads.append(pltpu.make_async_copy(wup_hbm, wup, ld_sem.at[4]))
    for h in range(2):
        cols = pl.ds(h * width, width)
        loads.append(pltpu.make_async_copy(wdown_hbm.at[:, cols], wdown.at[h], ld_sem.at[5 + h]))
    loads[0].start()

    barrier = pltpu.get_barrier_semaphore()
    for r in range(1, GROUP):
        pl.semaphore_signal(barrier, inc=1, device_id={"clip": partner[r]})
    pl.semaphore_signal(barrier, inc=1, device_id={"mp": peer})

    entry = [map_ref[s, me] for s in range(slots)]
    own = [jnp.where(e >= 0, lax.div(e, GROUP), -1) for e in entry]
    pick = []
    for r in range(GROUP):
        chosen = jnp.int32(0)
        for s in range(slots):
            chosen = jnp.where(own[s] == partner[r], s, chosen)
        pick.append(chosen)
    video = video_ref[me]
    mode = []
    for r in range(GROUP):
        m = jnp.int32(-1)
        for s in range(slots):
            e = map_ref[s, partner[r]]
            mine = (e >= 0) & (lax.div(e, GROUP) == me)
            m = jnp.where(mine, jnp.where(lax.rem(e, GROUP) < video, 0, 1), m)
        mode.append(m)

    place = [(GROUP - 1) * blk] + [(r - 1) * blk for r in range(1, GROUP)]
    span = [pl.ds(place[0], blk + EXTRA)] + [pl.ds(place[r], blk) for r in range(1, GROUP)]
    size = [blk + EXTRA] + [blk] * (GROUP - 1)

    def ici(r, src, dst, base):
        return pltpu.make_async_remote_copy(
            src_ref=src,
            dst_ref=dst,
            send_sem=send_sem.at[base + r],
            recv_sem=recv_sem.at[base + r],
            device_id={"clip": partner[r]},
        )

    def d2d(r, src, dst, base):
        return pltpu.make_async_remote_copy(
            src_ref=src,
            dst_ref=dst,
            send_sem=send_sem.at[base + r],
            recv_sem=recv_sem.at[base + r],
            device_id={"mp": peer},
        )

    half = x.at[core]
    arrive = [ici(r, snd.at[r - 1], half.at[span[r]], 0) if r else None for r in range(GROUP)]
    share = [d2d(r, half.at[span[r]], half.at[span[r]], 4) for r in range(GROUP)]
    proj = [d2d(r, ps1.at[span[r]], pr1.at[span[r]], 8) for r in range(GROUP)]
    joined = [d2d(r, aft.at[core].at[span[r]], aft.at[core].at[span[r]], 12) for r in range(GROUP)]
    down = [d2d(r, ps2.at[span[r]], pr2.at[span[r]], 16) for r in range(GROUP)]
    back = [ici(r, fin.at[r - 1], ret.at[r], 20) if r else None for r in range(GROUP)]

    loads[0].wait()
    for r in range(1, GROUP):
        snd[r - 1] = tok[pick[r]]
    x[core, pl.ds(place[0], blk)] = tok[pick[0]]
    small = bot_ref[0].astype(F32)
    for i in range(EXTRA // nb):
        ext[pl.ds(i * nb, nb)] = small
    x[core, pl.ds(total, EXTRA)] = ext[...].astype(BF16)

    pl.semaphore_wait(barrier, GROUP)
    for r in (1, 2, 3):
        arrive[r].start()
    share[0].start()
    for load in loads[1:]:
        load.start()

    column = lax.broadcasted_iota(jnp.int32, (1, keys), 1)
    extra_key = (column >= total) & (column < total + nb)
    key_mode = jnp.full((1, keys), -1, jnp.int32)
    for r in range(GROUP):
        inside = (column >= place[r]) & (column < place[r] + blk)
        key_mode = jnp.where(inside, mode[r], key_mode)

    def bias_of(m):
        return jnp.where(extra_key | ((key_mode == m) & (key_mode >= 0)), 0.0, NEG).astype(F32)

    row_bias = [bias_of(mode[r]) for r in range(GROUP)]
    bias[pl.ds(0, blk)] = jnp.broadcast_to(row_bias[0], (blk, keys))
    line = lax.broadcasted_iota(jnp.int32, (EXTRA, keys), 0)
    bias[pl.ds(blk, EXTRA)] = jnp.where(
        (line >= nb) & (line < 2 * nb),
        jnp.broadcast_to(bias_of(1), (EXTRA, keys)),
        jnp.broadcast_to(bias_of(0), (EXTRA, keys)),
    )
    for j in range(pairs):
        k[j, pl.ds(rows, keys - rows)] = jnp.zeros((keys - rows, 128), BF16)
        v[j, pl.ds(rows, keys - rows), :128] = jnp.zeros((keys - rows, 128), BF16)
        v[j, :, 128:] = jnp.ones((keys, 128), BF16)

    def project(r):
        n = layer_norm([x[0, span[r]], x[1, span[r]]], g1_ref[...])
        for i, target in enumerate((q, k, v)):
            y = dot(n, wqkv[i])
            if i == 0:
                y = y.astype(BF16).astype(F32) * HEAD_DIM ** (-0.5)
            y = y.astype(BF16)
            for j in range(pairs):
                target[j, span[r], :128] = y[:, j * 128 : (j + 1) * 128]

    loads[1].wait()
    share[0].wait_recv()
    project(0)
    for r in (1, 2):
        arrive[r].wait_recv()
        share[r].start()
    for r in (1, 2):
        share[r].wait_recv()
        project(r)
    arrive[3].wait_recv()
    share[3].start()
    share[3].wait_recv()
    project(3)

    def attend(r):
        lane = lax.broadcasted_iota(jnp.int32, (1, 128), 1)
        low = lane < HEAD_DIM

        def step(j, _):
            qs = q[j, span[r]]
            zero = jnp.zeros_like(qs)
            both = jnp.concatenate([jnp.where(low, qs, zero), jnp.where(low, zero, qs)], axis=0)
            s = lax.dot_general(both, k[j], (((1,), (1,)), ((), ())), preferred_element_type=F32)
            if r == 0:
                b = bias[...]
                s = s + jnp.concatenate([b, b], axis=0)
            else:
                s = s + row_bias[r]
            top = jnp.max(s, axis=-1, keepdims=True)
            p = jnp.exp(s - top).astype(BF16)
            o = dot(p, v[j])
            m = size[r]
            over = jnp.where(low, o[:m, :128], o[m:, :128])
            under = jnp.where(low, o[:m, 128:], o[m:, 128:])
            o = over / under
            if r == 0:
                ctx[j, pl.ds(place[0], blk)] = o[:blk].astype(BF16)
                e = o[blk:]
                e = 0.5 * (e + pltpu.roll(e, EXTRA - nb, 0))
                ctx[j, pl.ds(total, EXTRA)] = e.astype(BF16)
            else:
                ctx[j, span[r]] = o.astype(BF16)
            return 0

        lax.fori_loop(0, pairs, step, 0, unroll=UNROLL)

    def stage_a(r):
        attend(r)
        c = jnp.concatenate([ctx[j, span[r]] for j in range(pairs)], axis=1)
        ps1[span[r]] = dot(c, wout[peer]).astype(BF16)
        proj[r].start()
        own1[span[r]] = dot(c, wout[core])

    def stage_b(r):
        proj[r].wait_recv()
        total_sum = x[core, span[r]].astype(F32) + (own1[span[r]] + pr1[span[r]].astype(F32))
        aft[core, span[r]] = total_sum.astype(BF16)
        joined[r].start()

    def stage_c(r):
        joined[r].wait_recv()
        n = layer_norm([aft[0, span[r]], aft[1, span[r]]], g2_ref[...])
        tile = width
        for t in range(ff // tile):
            up = dot(n, wup[:, t * tile : (t + 1) * tile])
            act[pl.ds(0, size[r]), t * tile : (t + 1) * tile] = jax.nn.gelu(up, approximate=True).astype(BF16)
        a = act[pl.ds(0, size[r])]
        ps2[span[r]] = dot(a, wdown[peer]).astype(BF16)
        down[r].start()
        own2[span[r]] = dot(a, wdown[core])

    def stage_d(r):
        down[r].wait_recv()
        merged = aft[core, span[r]].astype(F32) + (own2[span[r]] + pr2[span[r]].astype(F32))
        if r == 0:
            ret[0] = merged[:blk].astype(BF16)
            outb_ref[0] = merged[blk : blk + nb].astype(BF16)
        else:
            fin[r - 1] = merged.astype(BF16)
            back[r].start()

    loads[2].wait()
    loads[3].wait()
    stage_a(3)
    stage_a(1)
    stage_b(3)
    stage_a(2)
    stage_b(1)
    for load in loads[4:]:
        load.wait()
    stage_c(3)
    stage_a(0)
    stage_b(2)
    stage_d(3)
    stage_c(1)
    stage_b(0)
    stage_d(1)
    stage_c(2)
    stage_d(2)
    stage_c(0)
    stage_d(0)
    for r in (3, 1, 2):
        back[r].wait_recv()
    for s in range(slots):
        where = jnp.int32(0)
        for r in range(GROUP):
            where = jnp.where(own[s] == partner[r], r, where)
        live = jnp.where(entry[s] >= 0, 1.0, 0.0).astype(F32)
        block = ret[where].astype(F32)
        out_ref[s] = (block * live).astype(BF16)
    for r in range(1, GROUP):
        arrive[r].wait_send()
        back[r].wait_send()
    for r in range(GROUP):
        for c in (share, proj, joined, down):
            c[r].wait_send()


def place(stored_ref, merged_ref, out_ref, outb_ref):
    out_ref[...] = stored_ref[...]
    outb_ref[...] = merged_ref[...]


def body(
    tokens,
    bottleneck,
    clip_lengths,
    video_blocks,
    store_map,
    norm1_gain,
    w_qkv,
    w_out,
    norm2_gain,
    w_up,
    w_down,
):
    slots, blk, width = tokens.shape
    nb = bottleneck.shape[1]
    dim = w_qkv.shape[1]
    inner = w_qkv.shape[2]
    ff = w_up.shape[1]
    pairs = inner // 128
    rows = GROUP * blk + EXTRA
    keys = (rows + 127) // 128 * 128
    smem = pl.BlockSpec(memory_space=pltpu.SMEM)
    vmem = pl.BlockSpec(memory_space=pltpu.VMEM)
    hbm = pl.BlockSpec(memory_space=pl.ANY)
    V = pltpu.VMEM
    stored, merged = pl.pallas_call(
        functools.partial(kernel, blk, nb),
        out_shape=(
            jax.ShapeDtypeStruct(tokens.shape, BF16),
            jax.ShapeDtypeStruct(bottleneck.shape, BF16),
        ),
        in_specs=[smem, smem, hbm, vmem, vmem, vmem, hbm, hbm, hbm, hbm],
        out_specs=(vmem, vmem),
        scratch_shapes=[
            V((slots, blk, width), BF16),
            V(w_qkv.shape, BF16),
            V((2, inner, width), BF16),
            V(w_up.shape, BF16),
            V((2, ff, width), BF16),
            V((GROUP - 1, blk, width), BF16),
            V((2, rows, width), BF16),
            V((EXTRA, width), F32),
            V((pairs, rows, 128), BF16),
            V((pairs, keys, 128), BF16),
            V((pairs, keys, 256), BF16),
            V((pairs, rows, 128), BF16),
            V((blk + EXTRA, keys), F32),
            V((rows, width), BF16),
            V((rows, width), BF16),
            V((rows, width), F32),
            V((2, rows, width), BF16),
            V((blk + EXTRA, ff), BF16),
            V((rows, width), BF16),
            V((rows, width), BF16),
            V((rows, width), F32),
            V((GROUP - 1, blk, width), BF16),
            V((GROUP, blk, width), BF16),
            pltpu.SemaphoreType.DMA((7,)),
            pltpu.SemaphoreType.DMA((24,)),
            pltpu.SemaphoreType.DMA((24,)),
        ],
        compiler_params=pltpu.CompilerParams(collective_id=0, has_side_effects=True),
        name="merge_layer",
    )(
        video_blocks,
        store_map.T,
        tokens,
        bottleneck,
        norm1_gain.reshape(1, dim),
        norm2_gain.reshape(1, dim),
        w_qkv,
        w_out,
        w_up,
        w_down,
    )
    return pl.pallas_call(
        place,
        out_shape=(
            jax.ShapeDtypeStruct(tokens.shape, BF16),
            jax.ShapeDtypeStruct(bottleneck.shape, BF16),
        ),
        in_specs=[vmem, vmem],
        out_specs=(vmem, vmem),
        name="place",
    )(stored, merged)


def solution(mesh):
    placed = (
        P("clip", None, "mp"),
        P("clip", None, "mp"),
        P(),
        P(),
        P(),
        P(),
        P(None, None, "mp"),
        P("mp", None),
        P(),
        P(None, "mp"),
        P("mp", None),
    )
    return jax.shard_map(
        body,
        mesh=mesh,
        in_specs=placed,
        out_specs=(P("clip", None, "mp"), P("clip", None, "mp")),
        check_vma=False,
    )
```
